32 devices in a mesh: section: 4 (over y, x), dp: 8 (over z, core).
Axes of the slice: x: 2, y: 2, z: 4, core: 2. Of those that a mesh axis runs over, the one named last changes fastest.
Arguments:
- descriptors: bfloat16 [4, 4096, 1024], P(None, 'dp'), may hold values from -6 to 6
- layer_weight: bfloat16 [4, 8, 1024, 1024], P('section', None, 'dp'), may hold values from -0.25 to 0.25
- layer_bias: float32 [4, 8, 1024], P('section'), may hold values from -3 to 3
- readout: float32 [8, 1024], replicated, may hold values from -0.75 to 0.75
- self_energy: float32 [8], replicated, may hold values from -2 to -0.5
- tile_species: int32 [4, 32], P(None, 'dp'), may hold values from 0 to 7
- tile_fill: int32 [4, 32], P(None, 'dp'), may hold values from 1 to 128
Outputs:
- atom_energy: float32 [4, 4096], P('section', 'dp')
- energy: float32 [4], replicated
The draws below stay inside these ranges and needn't reach their ends.
All inputs are finite; a program needn't handle non-finite values.
Results may differ from the reference program's by a relative error of at most 0.0044.
Values may be sent and summed in bfloat16 or wider, within the bound.
No kernel may reach another device: no remote copies, remote signals or barrier semaphores. Data moves between devices by JAX's collectives and lax.ppermute only.
A program may use at most 128 MiB of HBM per device.

```python
import jax
import jax.numpy as jnp
from jax import lax

H = 1024
SPECIES = 8
TILE = 128
SECTIONS = 4
MB = 4
TILES = 32
ATOMS = 4096


def set_ends(drawn, own_key, least, high):
    longest = drawn.shape.index(max(drawn.shape))
    spots = []
    for shift in (0, 1):
        where = [jax.random.randint(jax.random.fold_in(own_key, axis), (), 0, length) for axis, length in enumerate(drawn.shape)]
        where[longest] = (where[longest] + shift) % drawn.shape[longest]
        spots.append(tuple(where))
    return drawn.at[spots[0]].set(least).at[spots[1]].set(high)


def block_scale(stream_key, extent, cuts, low, high):
    level, own = 1.0, jax.random.fold_in(stream_key, 6)
    for position, parts in cuts:
        heights = jnp.exp(jax.random.uniform(jax.random.fold_in(own, position), (parts,), jnp.float32, low / len(cuts), high / len(cuts)))
        level = level * jnp.repeat(heights, extent[position] // parts).reshape([-1 if axis == position else 1 for axis in range(len(extent))])
    return level


def scatter_about(key, extent, spread, bound, shards=(), kind=jnp.bfloat16):
    entries = spread * jax.random.normal(key, extent, jnp.float32)
    if shards:
        entries = entries * block_scale(key, extent, shards, -0.22, 0.18)
    return jnp.clip(entries, -bound, bound).astype(kind)


def setup_inputs(seed: int = 0) -> dict:
    keys = jax.random.split(jax.random.key(seed), 8)
    return {
        "descriptors": scatter_about(keys[0], (MB, ATOMS, H), 1.0, 6.0, ((1, 8),)),
        "layer_weight": scatter_about(keys[1], (SECTIONS, SPECIES, H, H), (H // 2) ** -0.5, 0.25, ((0, 4), (2, 8))),
        "layer_bias": scatter_about(keys[2], (SECTIONS, SPECIES, H), 0.5, 3.0, ((0, 4),), jnp.float32),
        "readout": scatter_about(keys[3], (SPECIES, H), (H // 16) ** -0.5, 0.75, (), jnp.float32),
        "self_energy": jnp.clip(jax.random.uniform(keys[4], (SPECIES,), jnp.float32, -2.0, -0.5), -2.0, -0.5),
        "tile_species": set_ends(jax.random.randint(keys[5], (MB, TILES), 0, SPECIES), jax.random.fold_in(keys[5], 1), 0, SPECIES - 1).astype(jnp.int32),
        "tile_fill": set_ends(jax.random.randint(keys[6], (MB, TILES), 1, TILE + 1), jax.random.fold_in(keys[6], 1), 1, TILE).astype(jnp.int32),
    }


def smooth_unit(value):
    return jnp.maximum(value, 0.0) + jnp.minimum(jnp.expm1(jnp.minimum(value, 0.0)), 0.0)


def apply_layer(hidden, weight, bias, species):
    tiles = hidden.reshape(TILES, TILE, H)

    def one_tile(args):
        tile_rows, kind = args
        return jnp.dot(tile_rows, weight[kind], preferred_element_type=jnp.float32) + bias[kind][None, :]

    out = lax.map(one_tile, (tiles, species))
    return smooth_unit(out).reshape(ATOMS, H)


def reference(descriptors, layer_weight, layer_bias, readout, self_energy, tile_species, tile_fill):
    atom_rows = []
    totals = []
    slot = jnp.arange(ATOMS, dtype=jnp.int32) % TILE
    for batch in range(MB):
        species = tile_species[batch]
        hidden = descriptors[batch]
        active = None
        for layer in range(SECTIONS):
            active = apply_layer(hidden, layer_weight[layer], layer_bias[layer], species)
            if layer < SECTIONS - 1:
                hidden = active.astype(jnp.bfloat16)
        atom_kind = jnp.repeat(species, TILE)
        fill = jnp.repeat(tile_fill[batch], TILE)
        values = jnp.sum(active * readout[atom_kind], axis=-1) + self_energy[atom_kind]
        values = jnp.where(slot < fill, values, jnp.float32(0.0))
        atom_rows.append(values)
        totals.append(jnp.sum(values) / ATOMS)
    return jnp.stack(atom_rows), jnp.stack(totals)
```

```python
import functools

import jax
import jax.numpy as jnp
from jax import lax
from jax.experimental import pallas as pl
from jax.experimental.pallas import tpu as pltpu
from jax.sharding import PartitionSpec as P

GROUP = 2
SPLIT = 256


def pair_groups(devices, lanes):
    return [list(range(start, start + lanes)) for start in range(0, devices, lanes)]


def line_groups(devices, lanes):
    return [list(range(lane, devices, lanes)) for lane in range(lanes)]


def network(
    kind_ref, species_ref, fill_ref, self_ref, bias_ref, readout_ref, weight_hbm, *rest, sources, tile, layers
):
    tiles_hbm = rest[:sources]
    out_ref = rest[sources]
    weight, first, second, chosen, weight_sem, tile_sem = rest[sources + 1 :]
    positions, _, rows, width = weight_hbm.shape
    each = tiles_hbm[0].shape[0]
    kind = kind_ref[0]

    def weight_copy(layer, position):
        return pltpu.make_async_copy(
            weight_hbm.at[position, layer], weight.at[layer, pl.ds(position * rows, rows)], weight_sem.at[layer]
        )

    def tile_copy(source, index, slot):
        return pltpu.make_async_copy(
            tiles_hbm[source].at[index], first.at[pl.ds(slot * tile, tile)], tile_sem
        )

    count = jnp.int32(0)
    for source in range(sources):

        def pick(index, count, source=source):
            mine = species_ref[source * each + index] == kind

            @pl.when(mine)
            def _():
                chosen[count] = source * each + index
                tile_copy(source, index, count).start()

            return count + mine.astype(jnp.int32)

        count = lax.fori_loop(0, each, pick, count)
    for layer in range(layers):
        for position in range(positions):
            weight_copy(layer, position).start()
    out_ref[...] = jnp.zeros_like(out_ref)

    def settle(slot, carry):
        tile_copy(0, 0, slot).wait()
        return carry

    lax.fori_loop(0, count, settle, 0)
    groups = (count + GROUP - 1) // GROUP
    buffers = (first, second)
    for layer in range(layers):
        for position in range(positions):
            weight_copy(layer, position).wait()
        source, target = buffers[layer % 2], buffers[(layer + 1) % 2]
        is_last = layer == layers - 1

        def step(group, carry, layer=layer, source=source, target=target, is_last=is_last):
            begin = pl.multiple_of(group * (GROUP * tile), GROUP * tile)
            block = source[pl.ds(begin, GROUP * tile), :]
            sums = None
            for cut in range(0, width, SPLIT):
                value = jnp.dot(
                    block, weight[layer, :, cut : cut + SPLIT], preferred_element_type=jnp.float32
                )
                value = value + bias_ref[layer, :, cut : cut + SPLIT]
                active = jnp.maximum(value, jnp.exp(jnp.minimum(value, 0.0)) - 1.0)
                if not is_last:
                    target[pl.ds(begin, GROUP * tile), cut : cut + SPLIT] = active.astype(jnp.bfloat16)
                else:
                    terms = active * readout_ref[0, :, cut : cut + SPLIT]
                    for part in range(0, SPLIT, 128):
                        piece = terms[:, part : part + 128]
                        sums = piece if sums is None else sums + piece
            if is_last:
                for inner in range(GROUP):
                    slot = group * GROUP + inner
                    line = jnp.sum(sums[inner * tile : (inner + 1) * tile].T, axis=0, keepdims=True)
                    line = line + self_ref[0]

                    @pl.when(slot < count)
                    def _():
                        index = chosen[slot]
                        places = lax.broadcasted_iota(jnp.int32, (1, tile), 1)
                        out_ref[pl.ds(index, 1), :] = jnp.where(places < fill_ref[index], line, 0.0)

            return carry

        lax.fori_loop(0, groups, step, 0)


def energies_of(kind, species, fill, offset, bias, readout, weight, tile_sets):
    positions, layers, rows, width = weight.shape
    each, tile, _ = tile_sets[0].shape
    sources = len(tile_sets)
    slots = each * sources
    padded = -(-slots // GROUP) * GROUP
    smem = pl.BlockSpec(memory_space=pltpu.SMEM)
    vmem = pl.BlockSpec(memory_space=pltpu.VMEM)
    hbm = pl.BlockSpec(memory_space=pl.ANY)
    return pl.pallas_call(
        functools.partial(network, sources=sources, tile=tile, layers=layers),
        out_shape=jax.ShapeDtypeStruct((slots, tile), jnp.float32),
        in_specs=[smem, smem, smem, smem, vmem, vmem, hbm] + [hbm] * sources,
        out_specs=vmem,
        scratch_shapes=[
            pltpu.VMEM((layers, positions * rows, width), jnp.bfloat16),
            pltpu.VMEM((padded * tile, width), jnp.bfloat16),
            pltpu.VMEM((padded * tile, width), jnp.bfloat16),
            pltpu.SMEM((slots,), jnp.int32),
            pltpu.SemaphoreType.DMA((layers,)),
            pltpu.SemaphoreType.DMA,
        ],
        compiler_params=pltpu.CompilerParams(vmem_limit_bytes=56 * 1024 * 1024),
    )(kind, species, fill, offset, bias, readout, weight, *tile_sets)


def shards(descriptors, layer_weight, layer_bias, readout, self_energy, tile_species, tile_fill):
    sections = lax.axis_size("section")
    devices = lax.axis_size("dp")
    section = lax.axis_index("section")
    place = lax.axis_index("dp")
    batches, atoms_dev, width = descriptors.shape
    tiles_dev = tile_species.shape[1]
    tile = atoms_dev // tiles_dev
    kinds, rows = layer_weight.shape[1:3]
    lanes = kinds // sections
    positions = devices // lanes
    lane = place % lanes
    kind = section * lanes + lane
    pairs = pair_groups(devices, lanes)

    own = layer_weight[0].reshape(sections, lanes, rows, width)
    own = lax.all_to_all(own, "dp", 1, 1, tiled=True, axis_index_groups=pairs)
    own = lax.all_to_all(own, "section", 0, 0, tiled=True).reshape(sections, lanes * rows, width)
    weight = lax.all_gather(own, "dp", axis=0, axis_index_groups=line_groups(devices, lanes))

    bias = lax.all_gather(layer_bias[0], "section", axis=0)
    bias = lax.dynamic_index_in_dim(bias, kind, 1, keepdims=True)
    readout_row = lax.dynamic_index_in_dim(readout, kind, 0, keepdims=True)[None]
    offset = lax.dynamic_slice(self_energy, (kind,), (1,))

    table = jnp.stack([tile_species.reshape(-1), tile_fill.reshape(-1)])
    sets, tables = [], []
    mine = descriptors.reshape(batches * tiles_dev, tile, width)
    for turn in range(lanes):
        route = [(base[i], base[(i + turn) % lanes]) for base in pairs for i in range(lanes)]
        sets.append(lax.ppermute(mine, "dp", route) if turn else mine)
        tables.append(lax.ppermute(table, "dp", route) if turn else table)
    table = jnp.stack(tables, axis=1).reshape(2, -1)
    values = energies_of(kind[None], table[0], table[1], offset, bias, readout_row, weight, sets)
    values = values.reshape(lanes, batches, atoms_dev)
    partial = jnp.sum(values, axis=(0, 2)) / (atoms_dev * devices)

    order = (lane - jnp.arange(lanes)) % lanes
    values = jnp.take(values, order, axis=0)
    values = values.transpose(1, 0, 2)[:, None]
    here = (jnp.arange(positions) == place // lanes)[None, :, None, None]
    outgoing = jnp.where(here, values, 0.0)
    sums = jnp.broadcast_to(partial, outgoing.shape[:3] + (batches,))
    outgoing = jnp.concatenate([outgoing, sums], axis=-1).reshape(sections * devices, atoms_dev + batches)
    incoming = lax.all_to_all(outgoing, ("section", "dp"), 0, 0, tiled=True)
    total = jnp.sum(incoming, axis=0)
    return (total[None, :atoms_dev], total[atoms_dev:])


def solution(mesh):
    placed = (
        P(None, "dp", None),
        P("section", None, "dp", None),
        P("section", None, None),
        P(),
        P(),
        P(None, "dp"),
        P(None, "dp"),
    )
    return jax.shard_map(
        shards, mesh=mesh, in_specs=placed, out_specs=(P("section", "dp"), P()), check_vma=False
    )
```
